256 devices in a mesh: section: 8 (over z_hi, x), dp: 32 (over z_lo, y, core).
Axes of the slice: x: 4, y: 4, z: 8 (z_hi: 2, z_lo: 4; z = z_hi * 4 + z_lo), core: 2. Of those that a mesh axis runs over, the one named last changes fastest.
Arguments:
- features: bfloat16 [1, 8, 4096, 4096], P(None, 'section', 'dp'), parts along dimension 2, may hold values from -6 to 6
- in_proj: bfloat16 [8, 4096, 512], P('section'), may hold values from -0.09375 to 0.09375
- mix_proj: bfloat16 [8, 2, 256, 256], P('section'), may hold values from -0.375 to 0.375
- out_proj: bfloat16 [8, 512, 4096], P('section'), may hold values from -0.375 to 0.375
- gate_proj: bfloat16 [8, 2, 4096], P('section'), may hold values from -0.09375 to 0.09375
- cross_bias: float32 [8, 4096], P('section'), may hold values from -3 to 3
Outputs:
- crossed: bfloat16 [1, 8, 4096, 4096], P(None, 'section', 'dp'), parts along dimension 2
The draws below stay inside these ranges and needn't reach their ends.
There are 32 independent parts, one for each index of `dp`. The reference program is written for one: setup_inputs(seed, part) draws one part's arguments, and reference() takes and returns one part's arrays. A program takes and returns all parts, laid end to end along the dimension named above; an argument that names none is the same for every part. Nothing has to cross between parts.
All inputs are finite; a program needn't handle non-finite values.
Results may differ from the reference program's by a relative error of at most 0.015.
Values may be sent and summed in bfloat16 or wider, within the bound.
A program may use at most 64 MiB of HBM per device.

```python
import jax
import jax.numpy as jnp
from jax import lax

D = 4096
RANK = 256
EXPERTS = 2
ROWS = 128
MB_DEV = 1
LAYERS = 8
N_SECTION = 8


def shard_levels(own_key, shape, split, low, high):
    level = 1.0
    for dim, parts in split:
        steps = jax.random.uniform(jax.random.fold_in(jax.random.fold_in(own_key, 6), dim), (parts,), jnp.float32, low / len(split), high / len(split))
        level = level * jnp.repeat(jnp.exp(steps), shape[dim] // parts).reshape((-1,) + (1,) * (len(shape) - 1 - dim))
    return level


def centred(rng, extent, spread, reach, shards=(), kind=jnp.bfloat16):
    entries = spread * jax.random.normal(rng, extent, jnp.float32)
    if shards:
        entries = entries * shard_levels(rng, extent, shards, -0.22, 0.18)
    return jnp.clip(entries, -reach, reach).astype(kind)


def setup_inputs(seed: int = 0, part: int = 0) -> dict:
    arg_keys = jax.random.split(jax.random.key(seed), 7)
    part_splits = jax.random.split(jax.random.fold_in(arg_keys[6], part), 7)
    return {
        "features": centred(part_splits[0], (MB_DEV, N_SECTION, ROWS, D), 1.0, 6.0, ((1, 8),)),
        "in_proj": centred(arg_keys[1], (LAYERS, D, EXPERTS * RANK), D ** -0.5, 0.09375, ((0, 8),)),
        "mix_proj": centred(arg_keys[2], (LAYERS, EXPERTS, RANK, RANK), RANK ** -0.5, 0.375, ((0, 8),)),
        "out_proj": centred(arg_keys[3], (LAYERS, EXPERTS * RANK, D), RANK ** -0.5, 0.375, ((0, 8),)),
        "gate_proj": centred(arg_keys[4], (LAYERS, EXPERTS, D), D ** -0.5, 0.09375, ((0, 8),)),
        "cross_bias": centred(arg_keys[5], (LAYERS, D), 0.5, 3.0, ((0, 8),), jnp.float32),
    }


def cross_layer(current, anchor, v_mat, c_mat, u_mat, gate_mat, shift_row):
    row_count = current.shape[0]
    expert_count = c_mat.shape[0]
    rank_size = c_mat.shape[1]
    projected = jnp.dot(current, v_mat, preferred_element_type=jnp.float32)
    inner_first = jnp.tanh(projected).astype(jnp.bfloat16).reshape(row_count, expert_count, rank_size)
    inner_second = jnp.einsum("rek,ekj->rej", inner_first.astype(jnp.float32), c_mat.astype(jnp.float32))
    logits = lax.dot_general(current, gate_mat, (((1,), (1,)), ((), ())), preferred_element_type=jnp.float32)
    gate_values = 1.0 / jnp.sum(jnp.exp(logits[:, None, :] - logits[:, :, None]), axis=2)
    blended = (gate_values[:, :, None] * jnp.tanh(inner_second)).astype(jnp.bfloat16)
    blended = blended.reshape(row_count, expert_count * rank_size)
    crossed = jnp.dot(blended, u_mat, preferred_element_type=jnp.float32)
    updated = current.astype(jnp.float32) + anchor.astype(jnp.float32) * (crossed + shift_row)
    return updated.astype(jnp.bfloat16)


def reference(features, in_proj, mix_proj, out_proj, gate_proj, cross_bias):
    anchor = features.reshape(-1, features.shape[-1])
    current = anchor
    for level in range(LAYERS):
        current = cross_layer(current, anchor, in_proj[level], mix_proj[level], out_proj[level], gate_proj[level], cross_bias[level])
    return current.reshape(features.shape)
```

```python
import functools
import random

import jax
import jax.numpy as jnp
from jax import lax
from jax.experimental import pallas as pl
from jax.experimental.pallas import tpu as pltpu
from jax.sharding import PartitionSpec as P

MESH = pl.DeviceIdType.MESH
NX, NH, NK, NY, NQ = 4, 2, 4, 4, 2
NZ = NH * NK
LAYERS = NX * NH
CHUNKS = 17
LINKS = 5
LAG = 2
SLOTS = 4
NONE = 255
ORDER_WEIGHT, RARE_WEIGHT, NOISE, SEED = 0.6, 3.0, 0.5, 0


def plan_routes():
    rnd = random.Random(SEED)
    nodes = [(x, z, q) for x in range(NX) for z in range(NZ) for q in range(NQ)]
    index = {n: i for i, n in enumerate(nodes)}
    count = len(nodes)
    goes = []
    for x, z, q in nodes:
        goes.append([
            index[((x + 1) % NX, z, q)], index[((x - 1) % NX, z, q)],
            index[(x, (z + 1) % NZ, q)], index[(x, (z - 1) % NZ, q)], index[(x, z, 1 - q)],
        ])
    held = [{} for _ in nodes]
    copies = [0] * (LAYERS * CHUNKS)
    for u, (x, z, q) in enumerate(nodes):
        layer = z // NK * NX + x
        for c in range(CHUNKS):
            held[u][layer * CHUNKS + c] = 0
            copies[layer * CHUNKS + c] += 1
    missing = count * LAYERS * CHUNKS - sum(len(h) for h in held)
    sends, ready = [], [0] * LAYERS
    while missing:
        r = len(sends)
        row = [[NONE] * LINKS for _ in nodes]
        turns = [(u, o) for u in range(count) for o in range(LINKS)]
        rnd.shuffle(turns)
        now = list(copies)
        for u, o in turns:
            there = held[goes[u][o]]
            best, best_key = None, None
            for c, when in held[u].items():
                if when <= r and c not in there:
                    key = c // CHUNKS * ORDER_WEIGHT + now[c] / count * RARE_WEIGHT + rnd.random() * NOISE
                    if best_key is None or key < best_key:
                        best, best_key = c, key
            if best is not None:
                there[best] = r + LAG
                copies[best] += 1
                missing -= 1
                ready[best // CHUNKS] = max(ready[best // CHUNKS], r + LAG)
                row[u][o] = best % CHUNKS * LAYERS + best // CHUNKS
        sends.append(row)
    return nodes, goes, sends, ready


def route_tables():
    nodes, goes, sends, ready = plan_routes()
    rounds = len(sends) + LAG
    back = [1, 0, 3, 2, 4]
    out_table = [[[NONE] * LINKS for _ in nodes] for _ in range(rounds)]
    in_table = [[[NONE] * LINKS for _ in nodes] for _ in range(rounds)]
    for r, row in enumerate(sends):
        for u in range(len(nodes)):
            for o in range(LINKS):
                out_table[r][u][o] = row[u][o]
                in_table[r + LAG][goes[u][o]][back[o]] = row[u][o]
    return nodes, out_table, in_table, ready


def step_rounds(ready):
    starts, last = [], -1
    for layer in range(LAYERS):
        for half in range(2):
            last = max(last + 1, ready[layer] + (1 if half == 0 else 0))
            starts.append(last)
    starts += [last + 1, last + 2]
    return starts


def kernel(
    tables, v_hbm, u_hbm, c_hbm, e_hbm, feat_hbm, out_hbm,
    W, E, X0, XC, ACC, DACC, PS, PR, DS, DR, T_OUT, T_IN,
    local_sem, w_recv, e_recv, wd_recv, ed_recv, w_send, e_send, wd_send, ed_send,
    x_sem, p_send, p_recv, d_send, d_recv, o_local, o_send, o_recv,
):
    nodes, out_table, in_table, ready = tables
    rounds = len(out_table)
    starts = step_rounds(ready)
    total = max(rounds, starts[-1] + 1)
    rows, half = X0.shape[1], X0.shape[2]
    sub_cols, piece = half // 2, half // 4
    rank = piece // 2

    sec = lax.axis_index("section")
    dp = lax.axis_index("dp")
    x, h = sec % NX, sec // NX
    core, y, k = dp % 2, dp // 2 % NY, dp // (2 * NY)
    z = h * NK + k
    q = 1 - y % 2
    p = (y + 1) // 2 % 2
    mine = y % 2
    pair_y = y + 1 - 2 * mine
    share_y = (y + 1 - 2 * q + NY) % NY

    def device(x_, z_, y_, core_):
        return (z_ // NK * NX + x_, (z_ % NK * NY + y_) * 2 + core_)

    targets = [
        device((x + 1) % NX, z, y, core), device((x + NX - 1) % NX, z, y, core),
        device(x, (z + 1) % NZ, y, core), device(x, (z + NZ - 1) % NZ, y, core),
        device(x, z, share_y, core),
    ]
    pair = device(x, z, pair_y, core)
    sibling = device(x, z, y, 1 - core)

    def local(src, dst, sem):
        return pltpu.make_async_copy(src, dst, sem)

    def remote(src, dst, send, recv, to):
        return pltpu.make_async_remote_copy(
            src_ref=src, dst_ref=dst, send_sem=send, recv_sem=recv, device_id=to, device_id_type=MESH
        )

    def arrived(ref, sem):
        pltpu.make_async_copy(ref, ref, sem).wait()

    barrier = pltpu.get_barrier_semaphore()
    for to in targets + [pair, sibling]:
        pl.semaphore_signal(barrier, inc=1, device_id=to, device_id_type=MESH)

    base = pl.multiple_of(p * half, half)
    other = pl.multiple_of((1 - p) * half, half)
    own = []
    for s in range(2):
        for j in range(8):
            own.append(local(
                v_hbm.at[0, pl.ds(pl.multiple_of(base + s * sub_cols + j * 128, 128), 128), :],
                W.at[s, j, sec], local_sem.at[s, j]))
            b, a = j // 4, j % 4
            own.append(local(
                u_hbm.at[0, a * 128:(a + 1) * 128, pl.ds(pl.multiple_of(base + s * sub_cols + b * piece, piece), piece)],
                W.at[s, 8 + j, sec], local_sem.at[s, 8 + j]))
        own.append(local(c_hbm.at[s], W.at[s, 16, sec], local_sem.at[s, 16]))
        own.append(local(e_hbm.at[s], E.at[s, sec], local_sem.at[s, 17]))
    for copy in own:
        copy.start()
    x_local = local(feat_hbm.at[0, 0, :, pl.ds(base, half)], X0.at[mine], x_sem.at[0])
    x_local.start()

    bits = [x % 2 == 1, x // 2 == 1, h == 1, q == 1]
    shift = k * 8

    def lookup(table, r, o):
        values = {n: table[r][i][o] for i, n in enumerate(nodes)}
        words = []
        for cls in range(16):
            x_, h_, q_ = cls % 4, cls // 4 % 2, cls // 8
            word = 0
            for k_ in range(NK):
                word |= values[(x_, h_ * NK + k_, q_)] << (8 * k_)
            words.append(word - (1 << 32) if word >= 1 << 31 else word)
        level = words
        for bit in bits:
            level = [
                level[i] if isinstance(level[i], int) and isinstance(level[i + 1], int) and level[i] == level[i + 1]
                else jnp.where(bit, jnp.int32(level[i + 1]), jnp.int32(level[i]))
                for i in range(0, len(level), 2)
            ]
        word = level[0]
        if isinstance(word, int):
            word = jnp.int32(word)
        return lax.shift_right_logical(word, shift) & 255

    for r in range(rounds):
        for o in range(LINKS):
            T_OUT[r * LINKS + o] = lookup(out_table, r, o)
            T_IN[r * LINKS + o] = lookup(in_table, r, o)

    pl.semaphore_wait(barrier, LINKS + 2)
    x_remote = remote(feat_hbm.at[0, 0, :, pl.ds(other, half)], X0.at[mine], x_sem.at[1], x_sem.at[2], pair)
    x_remote.start()
    for copy in own:
        copy.wait()

    def settle(send_w, send_e, slot, ident):
        @pl.when(ident != NONE)
        def _():
            j, l = ident // LAYERS, ident % LAYERS
            arrived(W.at[core, j, l], send_w.at[slot])

            @pl.when(j == 16)
            def _():
                arrived(E.at[core, l], send_e.at[slot])

    def push(ident, slot, send_w, send_e, recv_w, recv_e, to):
        j, l = ident // LAYERS, ident % LAYERS
        remote(W.at[core, j, l], W.at[core, j, l], send_w.at[slot], recv_w.at[j, l], to).start()

        @pl.when(j == 16)
        def _():
            remote(E.at[core, l], E.at[core, l], send_e.at[slot], recv_e.at[l], to).start()

    def traffic(r):
        slot0 = r % SLOTS * LINKS

        @pl.when(r >= SLOTS)
        def _():
            for o in range(LINKS):
                settle(w_send, e_send, slot0 + o, T_OUT[(r - SLOTS) * LINKS + o])
                settle(wd_send, ed_send, slot0 + o, T_IN[(r - SLOTS) * LINKS + o])

        for o in range(LINKS):
            ident = T_IN[r * LINKS + o]

            @pl.when(ident != NONE)
            def _():
                j, l = ident // LAYERS, ident % LAYERS
                arrived(W.at[core, j, l], w_recv.at[j, l])

                @pl.when(j == 16)
                def _():
                    arrived(E.at[core, l], e_recv.at[l])

                push(ident, slot0 + o, wd_send, ed_send, wd_recv, ed_recv, sibling)

        for o in range(LINKS):
            ident_out = T_OUT[r * LINKS + o]

            @pl.when(ident_out != NONE)
            def _():
                push(ident_out, slot0 + o, w_send, e_send, w_recv, e_recv, targets[o])

    def weights_here(l):
        @pl.when(l != sec)
        def _():
            def one(j, carry):
                arrived(W.at[1 - core, j, l], wd_recv.at[j, l])
                return carry
            lax.fori_loop(0, CHUNKS, one, 0)
            arrived(E.at[1 - core, l], ed_recv.at[l])

    def project(l, s):
        acc = jnp.zeros((rows, piece), jnp.float32)
        mixed = jnp.zeros((rows, piece), jnp.float32)
        for sub in range(2):
            part = XC[s, :, sub * sub_cols:(sub + 1) * sub_cols]
            v_mat = W[sub, 0:8, l].reshape(sub_cols, piece)
            acc = acc + jnp.dot(part, v_mat, preferred_element_type=jnp.float32)
            for b in range(2):
                block = part[:, b * piece:(b + 1) * piece].astype(jnp.float32)
                mixed = mixed + block * E[sub, l, 2 + b:3 + b, :]
        ACC[s] = acc
        PS[l, s] = acc.astype(jnp.bfloat16)
        lanes = mixed[:, 0:128] + mixed[:, 128:256] + mixed[:, 256:384] + mixed[:, 384:512]
        logit = jnp.broadcast_to(jnp.sum(lanes, axis=1, keepdims=True), (rows, 128))
        DACC[s] = logit
        DS[l, s] = logit.T[0:8, :]
        remote(PS.at[l, s], PR.at[l, s], p_send.at[l, s], p_recv.at[l, s], pair).start()
        remote(DS.at[l, s], DR.at[l, s], d_send.at[l, s], d_recv.at[l, s], pair).start()

    def finish(l, s):
        arrived(PR.at[l, s], p_recv.at[l, s])
        arrived(DR.at[l, s], d_recv.at[l, s])
        first = jnp.tanh(ACC[s] + PR[l, s].astype(jnp.float32)).astype(jnp.bfloat16)
        logit = DACC[s] + jnp.broadcast_to(DR[l, s][0:1, :], (128, rows)).T
        gates = (1.0 / (1.0 + jnp.exp(-logit)), 1.0 / (1.0 + jnp.exp(logit)))
        c_mat = W[:, 16, l].reshape(rank, piece)
        parts = []
        for i in range(2):
            cols = slice(i * rank, (i + 1) * rank)
            second = jnp.dot(first[:, cols], c_mat[:, cols], preferred_element_type=jnp.float32)
            gate = jnp.concatenate([gates[i], gates[i]], axis=1)
            parts.append((gate * jnp.tanh(second)).astype(jnp.bfloat16))
        blended = jnp.concatenate(parts, axis=1)
        for sub in range(2):
            for b in range(2):
                u_mat = W[sub, 8 + 4 * b:12 + 4 * b, l].reshape(piece, piece)
                cross = jnp.dot(blended, u_mat, preferred_element_type=jnp.float32)
                at = sub * sub_cols + b * piece
                cols = slice(at, at + piece)
                new = XC[s, :, cols].astype(jnp.float32) + X0[s, :, cols].astype(jnp.float32) * (
                    cross + E[sub, l, b:b + 1, :])
                XC[s, :, cols] = new.astype(jnp.bfloat16)

                @pl.when(l == LAYERS - 1)
                def _():
                    j = sub * 2 + b
                    dst = out_hbm.at[0, 0, :, pl.ds(pl.multiple_of(base + at, piece), piece)]

                    @pl.when(s == mine)
                    def _():
                        local(XC.at[s, :, cols], dst, o_local.at[j]).start()

                    @pl.when(s != mine)
                    def _():
                        remote(XC.at[s, :, cols], dst, o_send.at[j], o_recv.at[j], pair).start()

    def one_round(r, carry):
        @pl.when(r < rounds)
        def _():
            traffic(r)

        step = jnp.int32(-1)
        fires = jnp.int32(0)
        for start in starts:
            step = step + jnp.where(r >= start, 1, 0)
            fires = fires + jnp.where(r == start, 1, 0)

        @pl.when(fires > 0)
        def _():
            l, s = step // 2, step % 2

            @pl.when(step == 0)
            def _():
                x_local.wait()
                x_remote.wait_send()
                arrived(X0.at[1 - mine], x_sem.at[2])
                XC[...] = X0[...]

            @pl.when(step >= 2)
            def _():
                finish(l - 1, s)

            @pl.when(l < LAYERS)
            def _():
                @pl.when(s == 0)
                def _():
                    weights_here(l)
                project(l, s)

        return carry

    lax.fori_loop(0, total, one_round, 0)

    for r in range(max(rounds - SLOTS, 0), rounds):
        for o in range(LINKS):
            slot = r % SLOTS * LINKS + o
            settle(w_send, e_send, slot, T_OUT[r * LINKS + o])
            settle(wd_send, ed_send, slot, T_IN[r * LINKS + o])

    def sent(i, carry):
        l, s = i // 2, i % 2
        arrived(PS.at[l, s], p_send.at[l, s])
        arrived(DS.at[l, s], d_send.at[l, s])
        return carry

    lax.fori_loop(0, LAYERS * 2, sent, 0)
    for j in range(4):
        at = j * piece
        cols = slice(at, at + piece)
        mine_dst = out_hbm.at[0, 0, :, pl.ds(pl.multiple_of(base + at, piece), piece)]
        pair_dst = out_hbm.at[0, 0, :, pl.ds(pl.multiple_of(other + at, piece), piece)]
        local(XC.at[mine, :, cols], mine_dst, o_local.at[j]).wait()
        arrived(XC.at[1 - mine, :, cols], o_send.at[j])
        arrived(pair_dst, o_recv.at[j])


def per_device(features, in_proj, mix_proj, out_proj, gate_proj, cross_bias):
    rows, width = features.shape[2], features.shape[3]
    experts, rank = mix_proj.shape[1], mix_proj.shape[2]
    half, piece = width // 2, experts * rank
    y = lax.axis_index("dp") // 2 % NY
    p = (y + 1) // 2 % 2

    def own_half(vector):
        return lax.dynamic_slice_in_dim(vector.reshape(2, 2, 2, piece), p, 1, axis=0)[0]

    gate = gate_proj[0].astype(jnp.float32)
    extra = jnp.concatenate(
        [own_half(cross_bias[0]), own_half(gate[0] - gate[1]), jnp.zeros((2, 4, piece), jnp.float32)], axis=1
    )
    mix = mix_proj[0].transpose(1, 0, 2).reshape(2, rank // 2, piece)
    tables = route_tables()
    rounds = len(tables[1])
    any_space = pl.BlockSpec(memory_space=pl.ANY)
    dma = pltpu.SemaphoreType.DMA
    return pl.pallas_call(
        functools.partial(kernel, tables),
        out_shape=jax.ShapeDtypeStruct(features.shape, features.dtype),
        in_specs=[any_space] * 5,
        out_specs=any_space,
        scratch_shapes=[
            pltpu.VMEM((2, CHUNKS, LAYERS, 128, piece), jnp.bfloat16),
            pltpu.VMEM((2, LAYERS, 8, piece), jnp.float32),
            pltpu.VMEM((2, rows, half), jnp.bfloat16),
            pltpu.VMEM((2, rows, half), jnp.bfloat16),
            pltpu.VMEM((2, rows, piece), jnp.float32),
            pltpu.VMEM((2, rows, 128), jnp.float32),
            pltpu.VMEM((LAYERS, 2, rows, piece), jnp.bfloat16),
            pltpu.VMEM((LAYERS, 2, rows, piece), jnp.bfloat16),
            pltpu.VMEM((LAYERS, 2, 8, rows), jnp.float32),
            pltpu.VMEM((LAYERS, 2, 8, rows), jnp.float32),
            pltpu.SMEM((rounds * LINKS,), jnp.int32),
            pltpu.SMEM((rounds * LINKS,), jnp.int32),
            dma((2, 18)),
            dma((CHUNKS, LAYERS)), dma((LAYERS,)),
            dma((CHUNKS, LAYERS)), dma((LAYERS,)),
            dma((SLOTS * LINKS,)), dma((SLOTS * LINKS,)),
            dma((SLOTS * LINKS,)), dma((SLOTS * LINKS,)),
            dma((3,)),
            dma((LAYERS, 2)), dma((LAYERS, 2)), dma((LAYERS, 2)), dma((LAYERS, 2)),
            dma((4,)), dma((4,)), dma((4,)),
        ],
        compiler_params=pltpu.CompilerParams(
            collective_id=0, has_side_effects=True, vmem_limit_bytes=60 * 1024 * 1024
        ),
    )(in_proj, out_proj, mix, extra, features)


def solution(mesh):
    placed = (
        P(None, "section", "dp", None),
        P("section", None, None),
        P("section", None, None, None),
        P("section", None, None),
        P("section", None, None),
        P("section", None),
    )
    return jax.shard_map(
        per_device,
        mesh=mesh,
        in_specs=placed,
        out_specs=P(None, "section", "dp", None),
        check_vma=False,
    )
```

```python
import functools
import random

import jax
import jax.numpy as jnp
from jax import lax
from jax.experimental import pallas as pl
from jax.experimental.pallas import tpu as pltpu
from jax.sharding import PartitionSpec as P

MESH = pl.DeviceIdType.MESH
NX, NH, NK, NY, NQ = 4, 2, 4, 4, 2
NZ = NH * NK
LAYERS = NX * NH
PART = 128
NV = 1024 // PART
NC = 128 // PART
CHUNKS = 2 * NV + NC
LINKS = 5
LAG = 2
PACE, GAP = 1, 1
SLOTS = 4
NONE = 4095
ROUTE = (0.8, 4, 0.3, 3600, 2, 2)


def chunk_groups():
    first = list(range(NV)) + list(range(2 * NV, CHUNKS))
    return first, list(range(NV, NV + NV // 2)), list(range(NV + NV // 2, 2 * NV))


def plan_routes(order_weight, rare_weight, noise, seed, late, last):
    rnd = random.Random(seed)
    nodes = [(x, z, q) for x in range(NX) for z in range(NZ) for q in range(NQ)]
    index = {n: i for i, n in enumerate(nodes)}
    count = len(nodes)
    goes = []
    for x, z, q in nodes:
        goes.append([
            index[((x + 1) % NX, z, q)], index[((x - 1) % NX, z, q)],
            index[(x, (z + 1) % NZ, q)], index[(x, (z - 1) % NZ, q)], index[(x, z, 1 - q)],
        ])
    _, second, third = chunk_groups()
    due = []
    for c in range(LAYERS * CHUNKS):
        layer, part = divmod(c, CHUNKS)
        steps = 2 * layer + (late if part in second + third else 0)
        if layer == LAYERS - 1 and part in third:
            steps += last
        due.append(steps * order_weight / 2)
    held = [{} for _ in nodes]
    copies = [0] * (LAYERS * CHUNKS)
    for u, (x, z, q) in enumerate(nodes):
        layer = z // NK * NX + x
        for c in range(CHUNKS):
            held[u][layer * CHUNKS + c] = 0
            copies[layer * CHUNKS + c] += 1
    missing = count * LAYERS * CHUNKS - sum(len(h) for h in held)
    sends, ready = [], [0] * (LAYERS * CHUNKS)
    while missing:
        r = len(sends)
        row = [[NONE] * LINKS for _ in nodes]
        turns = [(u, o) for u in range(count) for o in range(LINKS)]
        rnd.shuffle(turns)
        base = [due[c] + copies[c] / count * rare_weight for c in range(LAYERS * CHUNKS)]
        for u, o in turns:
            there = held[goes[u][o]]
            best, best_key = None, None
            for c, when in held[u].items():
                if when <= r and c not in there:
                    key = base[c] + rnd.random() * noise
                    if best_key is None or key < best_key:
                        best, best_key = c, key
            if best is not None:
                there[best] = r + LAG
                copies[best] += 1
                missing -= 1
                ready[best] = max(ready[best], r + LAG)
                row[u][o] = best % CHUNKS * LAYERS + best // CHUNKS
        sends.append(row)
    return nodes, goes, sends, ready


def route_tables():
    nodes, goes, sends, ready = plan_routes(*ROUTE)
    rounds = len(sends) + LAG
    back = [1, 0, 3, 2, 4]
    out_table = [[[NONE] * LINKS for _ in nodes] for _ in range(rounds)]
    in_table = [[[NONE] * LINKS for _ in nodes] for _ in range(rounds)]
    for r, row in enumerate(sends):
        for u in range(len(nodes)):
            for o in range(LINKS):
                out_table[r][u][o] = row[u][o]
                in_table[r + LAG][goes[u][o]][back[o]] = row[u][o]
    return nodes, out_table, in_table, step_rounds(ready)


def step_rounds(ready):
    def last_of(layer, group):
        return max(ready[layer * CHUNKS + c] for c in group)

    first, second, third = chunk_groups()
    pace, gap = PACE, GAP
    starts, at = [], -pace
    for layer in range(LAYERS):
        need = last_of(layer, first) + gap
        if layer:
            need = max(need, last_of(layer - 1, second + third) + gap)
        at = max(at + pace, need)
        starts.append(at)
        at += pace
        starts.append(at)
    starts += [at + pace, at + 2 * pace]
    at = max(at + 2 * pace + 1, last_of(LAYERS - 1, second) + gap)
    starts.append(at)
    starts.append(max(at + 1, last_of(LAYERS - 1, third) + gap))
    return starts


def kernel(
    tables, v_hbm, u_hbm, c_hbm, gate_ref, bias_ref, feat_hbm, out_hbm,
    W, E, X0, XC, ACC, DACC, BL, PS, PR, DS, DR, T_OUT, T_IN,
    local_sem, w_recv, e_recv, wd_recv, ed_recv, w_send, e_send, wd_send, ed_send,
    x_sem, p_send, p_recv, d_send, d_recv, o_local, o_send, o_recv,
):
    nodes, out_table, in_table, starts = tables
    rounds = len(out_table)
    total = max(rounds, starts[-1] + 1)
    rows, half = X0.shape[1], X0.shape[2]
    sub_cols, piece = half // 2, half // 4
    rank = piece // 2
    block = rows // 2
    deep = piece // PART

    sec = lax.axis_index("section")
    dp = lax.axis_index("dp")
    x, h = sec % NX, sec // NX
    core, y, k = dp % 2, dp // 2 % NY, dp // (2 * NY)
    z = h * NK + k
    q = 1 - y % 2
    p = (y + 1) // 2 % 2
    mine = y % 2
    pair_y = y + 1 - 2 * mine
    share_y = (y + 1 - 2 * q + NY) % NY

    def device(x_, z_, y_, core_):
        return (z_ // NK * NX + x_, (z_ % NK * NY + y_) * 2 + core_)

    targets = [
        device((x + 1) % NX, z, y, core), device((x + NX - 1) % NX, z, y, core),
        device(x, (z + 1) % NZ, y, core), device(x, (z + NZ - 1) % NZ, y, core),
        device(x, z, share_y, core),
    ]
    pair = device(x, z, pair_y, core)
    sibling = device(x, z, y, 1 - core)

    def local(src, dst, sem):
        return pltpu.make_async_copy(src, dst, sem)

    def remote(src, dst, send, recv, to):
        return pltpu.make_async_remote_copy(
            src_ref=src, dst_ref=dst, send_sem=send, recv_sem=recv, device_id=to, device_id_type=MESH
        )

    def arrived(ref, sem):
        pltpu.make_async_copy(ref, ref, sem).wait()

    barrier = pltpu.get_barrier_semaphore()
    for to in targets + [pair, sibling]:
        pl.semaphore_signal(barrier, inc=1, device_id=to, device_id_type=MESH)

    base = pl.multiple_of(p * half, half)
    other = pl.multiple_of((1 - p) * half, half)
    own = []
    for s in range(2):
        for j in range(NV):
            own.append(local(
                v_hbm.at[0, pl.ds(pl.multiple_of(base + s * sub_cols + j * PART, PART), PART), :],
                W.at[s, j, sec], local_sem.at[s, j]))
            b, a = j // deep, j % deep
            own.append(local(
                u_hbm.at[0, a * PART:(a + 1) * PART, pl.ds(pl.multiple_of(base + s * sub_cols + b * piece, piece), piece)],
                W.at[s, NV + j, sec], local_sem.at[s, NV + j]))
        for j in range(NC):
            for e in range(2):
                own.append(local(
                    c_hbm.at[0, e, s * 128 + j * PART:s * 128 + (j + 1) * PART, :],
                    W.at[s, 2 * NV + j, sec, :, e * rank:(e + 1) * rank], local_sem.at[s, 2 * NV + 2 * j + e]))
    for copy in own:
        copy.start()
    x_local = [
        local(feat_hbm.at[0, 0, s * block:(s + 1) * block, pl.ds(base, half)],
              X0.at[s, pl.ds(pl.multiple_of(mine * block, block), block), :], x_sem.at[s])
        for s in range(2)
    ]
    for copy in x_local:
        copy.start()
    for s in range(2):
        extra = []
        for ref in (bias_ref, gate_ref):
            for b in range(2):
                cols = pl.ds(pl.multiple_of(base + s * sub_cols + b * piece, piece), piece)
                if ref is bias_ref:
                    extra.append(ref[0:1, cols])
                else:
                    both = ref[0, :, cols].astype(jnp.float32)
                    extra.append(both[0:1, :] - both[1:2, :])
        extra.append(jnp.zeros((4, piece), jnp.float32))
        E[s, sec] = jnp.concatenate(extra, axis=0)

    bits = [x % 2 == 1, x // 2 == 1, h == 1, q == 1, k // 2 == 1]
    shift = k % 2 * 16

    def lookup(table, r, o):
        values = {n: table[r][i][o] for i, n in enumerate(nodes)}
        level = []
        for cls in range(32):
            x_, h_, q_, k_ = cls % 4, cls // 4 % 2, cls // 8 % 2, cls // 16 * 2
            level.append(values[(x_, h_ * NK + k_, q_)] + (values[(x_, h_ * NK + k_ + 1, q_)] << 16))
        for bit in bits:
            level = [
                level[i] if isinstance(level[i], int) and isinstance(level[i + 1], int) and level[i] == level[i + 1]
                else jnp.where(bit, jnp.int32(level[i + 1]), jnp.int32(level[i]))
                for i in range(0, len(level), 2)
            ]
        word = level[0]
        if isinstance(word, int):
            word = jnp.int32(word)
        return lax.shift_right_logical(word, shift) & 4095

    for r in range(rounds):
        for o in range(LINKS):
            T_OUT[r * LINKS + o] = lookup(out_table, r, o)
            T_IN[r * LINKS + o] = lookup(in_table, r, o)

    pl.semaphore_wait(barrier, LINKS + 2)
    x_remote = [
        remote(feat_hbm.at[0, 0, s * block:(s + 1) * block, pl.ds(other, half)],
               X0.at[s, pl.ds(pl.multiple_of(mine * block, block), block), :], x_sem.at[2 + s], x_sem.at[4 + s], pair)
        for s in range(2)
    ]
    for copy in x_remote:
        copy.start()
    for copy in own:
        copy.wait()

    def settle(send_w, send_e, slot, ident):
        @pl.when(ident != NONE)
        def _():
            j, l = ident // LAYERS, ident % LAYERS
            arrived(W.at[core, j, l], send_w.at[slot])

            @pl.when(j == 2 * NV)
            def _():
                arrived(E.at[core, l], send_e.at[slot])

    def push(ident, slot, send_w, send_e, recv_w, recv_e, to):
        j, l = ident // LAYERS, ident % LAYERS
        remote(W.at[core, j, l], W.at[core, j, l], send_w.at[slot], recv_w.at[j, l], to).start()

        @pl.when(j == 2 * NV)
        def _():
            remote(E.at[core, l], E.at[core, l], send_e.at[slot], recv_e.at[l], to).start()

    def traffic(r):
        slot0 = r % SLOTS * LINKS

        @pl.when(r >= SLOTS)
        def _():
            for o in range(LINKS):
                settle(w_send, e_send, slot0 + o, T_OUT[(r - SLOTS) * LINKS + o])
                settle(wd_send, ed_send, slot0 + o, T_IN[(r - SLOTS) * LINKS + o])

        for o in range(LINKS):
            ident = T_IN[r * LINKS + o]

            @pl.when(ident != NONE)
            def _():
                j, l = ident // LAYERS, ident % LAYERS
                arrived(W.at[core, j, l], w_recv.at[j, l])

                @pl.when(j == 2 * NV)
                def _():
                    arrived(E.at[core, l], e_recv.at[l])

                push(ident, slot0 + o, wd_send, ed_send, wd_recv, ed_recv, sibling)

        for o in range(LINKS):
            ident_out = T_OUT[r * LINKS + o]

            @pl.when(ident_out != NONE)
            def _():
                push(ident_out, slot0 + o, w_send, e_send, w_recv, e_recv, targets[o])

    def weights_here(l, low, high, extra=False):
        @pl.when(l != sec)
        def _():
            def one(j, carry):
                arrived(W.at[1 - core, j, l], wd_recv.at[j, l])
                return carry
            lax.fori_loop(low, high, one, 0)
            if extra:
                arrived(E.at[1 - core, l], ed_recv.at[l])

    def project(l, s):
        acc = jnp.zeros((rows, piece), jnp.float32)
        mixed = jnp.zeros((rows, piece), jnp.float32)
        for sub in range(2):
            part = XC[s, :, sub * sub_cols:(sub + 1) * sub_cols]
            v_mat = W[sub, 0:NV, l].reshape(sub_cols, piece)
            acc = acc + jnp.dot(part, v_mat, preferred_element_type=jnp.float32)
            for b in range(2):
                cut = part[:, b * piece:(b + 1) * piece].astype(jnp.float32)
                mixed = mixed + cut * E[sub, l, 2 + b:3 + b, :]
        ACC[s] = acc
        PS[l, s] = acc.astype(jnp.bfloat16)
        lanes = mixed[:, 0:128] + mixed[:, 128:256] + mixed[:, 256:384] + mixed[:, 384:512]
        logit = jnp.broadcast_to(jnp.sum(lanes, axis=1, keepdims=True), (rows, 128))
        DACC[s] = logit
        DS[l, s] = logit.T[0:8, :]
        remote(PS.at[l, s], PR.at[l, s], p_send.at[l, s], p_recv.at[l, s], pair).start()
        remote(DS.at[l, s], DR.at[l, s], d_send.at[l, s], d_recv.at[l, s], pair).start()

    def blend(l, s):
        arrived(PR.at[l, s], p_recv.at[l, s])
        arrived(DR.at[l, s], d_recv.at[l, s])
        first = jnp.tanh(ACC[s] + PR[l, s].astype(jnp.float32)).astype(jnp.bfloat16)
        logit = DACC[s] + jnp.broadcast_to(DR[l, s][0:1, :], (128, rows)).T
        gates = (1.0 / (1.0 + jnp.exp(-logit)), 1.0 / (1.0 + jnp.exp(logit)))
        c_mat = W[:, 2 * NV:CHUNKS, l].reshape(rank, piece)
        parts = []
        for i in range(2):
            cols = slice(i * rank, (i + 1) * rank)
            second = jnp.dot(first[:, cols], c_mat[:, cols], preferred_element_type=jnp.float32)
            gate = jnp.concatenate([gates[i], gates[i]], axis=1)
            parts.append((gate * jnp.tanh(second)).astype(jnp.bfloat16))
        return jnp.concatenate(parts, axis=1)

    def expand(blended, l, s, sub, b):
        u_mat = W[sub, pl.ds(NV + deep * b, deep), l].reshape(piece, piece)
        cross = jnp.dot(blended, u_mat, preferred_element_type=jnp.float32)
        cols = pl.ds(pl.multiple_of(sub * sub_cols + b * piece, piece), piece)
        new = XC[s, :, cols].astype(jnp.float32) + X0[s, :, cols].astype(jnp.float32) * (
            cross + E[sub, l, pl.ds(b, 1), :])
        XC[s, :, cols] = new.astype(jnp.bfloat16)

    def finish(l, s):
        blended = blend(l, s)
        for sub in range(2):
            for b in range(2):
                expand(blended, l, s, sub, b)

    def results(b, s, sub):
        at = sub * sub_cols + b * piece
        src = pl.ds(pl.multiple_of(at, piece), piece)
        dst = out_hbm.at[0, 0, s * block:(s + 1) * block, pl.ds(pl.multiple_of(base + at, piece), piece)]
        slot = b * 4 + s * 2 + sub
        return (
            local(XC.at[s, pl.ds(pl.multiple_of(mine * block, block), block), src], dst, o_local.at[slot]),
            remote(XC.at[s, pl.ds(pl.multiple_of((1 - mine) * block, block), block), src], dst,
                   o_send.at[slot], o_recv.at[slot], pair),
        )

    def one_round(r, carry):
        @pl.when(r < rounds)
        def _():
            traffic(r)

        step = jnp.int32(-1)
        fires = jnp.int32(0)
        for start in starts:
            step = step + jnp.where(r >= start, 1, 0)
            fires = fires + jnp.where(r == start, 1, 0)

        @pl.when((fires > 0) & (step < 2 * LAYERS))
        def _():
            l, s = step // 2, step % 2

            @pl.when(step == 0)
            def _():
                for copy in x_local:
                    copy.wait()
                for s_ in range(2):
                    x_remote[s_].wait_send()
                    arrived(X0.at[s_, pl.ds(pl.multiple_of((1 - mine) * block, block), block), :], x_sem.at[4 + s_])
                XC[...] = X0[...]

            @pl.when(step >= 2)
            def _():
                @pl.when(s == 0)
                def _():
                    weights_here(l - 1, NV, 2 * NV)
                finish(l - 1, s)

            @pl.when(s == 0)
            def _():
                weights_here(l, 0, NV)
                weights_here(l, 2 * NV, CHUNKS, True)
            project(l, s)

        @pl.when((fires > 0) & (step >= 2 * LAYERS) & (step < 2 * LAYERS + 2))
        def _():
            BL[step % 2] = blend(LAYERS - 1, step % 2)

        @pl.when((fires > 0) & (step >= 2 * LAYERS + 2))
        def _():
            b = step % 2
            low = NV + b * (NV // 2)
            weights_here(LAYERS - 1, low, low + NV // 2)
            for s in range(2):
                for sub in range(2):
                    expand(BL[s], LAYERS - 1, s, sub, b)
                    for copy in results(b, s, sub):
                        copy.start()

        return carry

    lax.fori_loop(0, total, one_round, 0)

    for r in range(max(rounds - SLOTS, 0), rounds):
        for o in range(LINKS):
            slot = r % SLOTS * LINKS + o
            settle(w_send, e_send, slot, T_OUT[r * LINKS + o])
            settle(wd_send, ed_send, slot, T_IN[r * LINKS + o])

    def sent(i, carry):
        l, s = i // 2, i % 2
        arrived(PS.at[l, s], p_send.at[l, s])
        arrived(DS.at[l, s], d_send.at[l, s])
        return carry

    lax.fori_loop(0, LAYERS * 2, sent, 0)
    for b in range(2):
        for s in range(2):
            for sub in range(2):
                here, there = results(b, s, sub)
                here.wait()
                there.wait_send()
                at = sub * sub_cols + b * piece
                arrived(out_hbm.at[0, 0, s * block:(s + 1) * block, pl.ds(pl.multiple_of(other + at, piece), piece)],
                        o_recv.at[b * 4 + s * 2 + sub])


def per_device(features, in_proj, mix_proj, out_proj, gate_proj, cross_bias):
    rows, width = features.shape[2], features.shape[3]
    experts, rank = mix_proj.shape[1], mix_proj.shape[2]
    half, piece = width // 2, experts * rank
    tables = route_tables()
    rounds = len(tables[1])
    any_space = pl.BlockSpec(memory_space=pl.ANY)
    dma = pltpu.SemaphoreType.DMA
    return pl.pallas_call(
        functools.partial(kernel, tables),
        out_shape=jax.ShapeDtypeStruct(features.shape, features.dtype),
        in_specs=[any_space] * 3 + [pl.BlockSpec(memory_space=pltpu.VMEM)] * 2 + [any_space],
        out_specs=any_space,
        scratch_shapes=[
            pltpu.VMEM((2, CHUNKS, LAYERS, PART, piece), jnp.bfloat16),
            pltpu.VMEM((2, LAYERS, 8, piece), jnp.float32),
            pltpu.VMEM((2, rows, half), jnp.bfloat16),
            pltpu.VMEM((2, rows, half), jnp.bfloat16),
            pltpu.VMEM((2, rows, piece), jnp.float32),
            pltpu.VMEM((2, rows, 128), jnp.float32),
            pltpu.VMEM((2, rows, piece), jnp.bfloat16),
            pltpu.VMEM((LAYERS, 2, rows, piece), jnp.bfloat16),
            pltpu.VMEM((LAYERS, 2, rows, piece), jnp.bfloat16),
            pltpu.VMEM((LAYERS, 2, 8, rows), jnp.float32),
            pltpu.VMEM((LAYERS, 2, 8, rows), jnp.float32),
            pltpu.SMEM((rounds * LINKS,), jnp.int32),
            pltpu.SMEM((rounds * LINKS,), jnp.int32),
            dma((2, CHUNKS + NC)),
            dma((CHUNKS, LAYERS)), dma((LAYERS,)),
            dma((CHUNKS, LAYERS)), dma((LAYERS,)),
            dma((SLOTS * LINKS,)), dma((SLOTS * LINKS,)),
            dma((SLOTS * LINKS,)), dma((SLOTS * LINKS,)),
            dma((6,)),
            dma((LAYERS, 2)), dma((LAYERS, 2)), dma((LAYERS, 2)), dma((LAYERS, 2)),
            dma((8,)), dma((8,)), dma((8,)),
        ],
        compiler_params=pltpu.CompilerParams(
            collective_id=0, has_side_effects=True, vmem_limit_bytes=60 * 1024 * 1024
        ),
    )(in_proj, out_proj, mix_proj, gate_proj, cross_bias, features)


def solution(mesh):
    placed = (
        P(None, "section", "dp", None),
        P("section", None, None),
        P("section", None, None, None),
        P("section", None, None),
        P("section", None, None),
        P("section", None),
    )
    return jax.shard_map(
        per_device,
        mesh=mesh,
        in_specs=placed,
        out_specs=P(None, "section", "dp", None),
        check_vma=False,
    )
```

```python
import functools

import jax
import jax.numpy as jnp
import numpy as np
from jax import lax
from jax.experimental import pallas as pl
from jax.experimental.pallas import tpu as pltpu
from jax.sharding import PartitionSpec as P

MESH = pl.DeviceIdType.MESH
NX, NH, NK, NY, NQ = 4, 2, 4, 4, 2
NZ = NH * NK
LAYERS = NX * NH
PART = 128
NV = 1024 // PART
NC = 128 // PART
CHUNKS = 2 * NV + NC
LINKS = 5
LAG = 2
PACE = 1.0
SLOTS = 4
NONE = 4095
DUE = [
    [[0.0, 0.5], [0.5849288578929801, 0.75], [0.9381583654646382, 1.42876989990142], [1.5, 1.75], [2.049650217767926, 2.430761940989174], [2.640286836685923, 2.90658948692369], [3.08954911142396, 3.24213595349004], [3.519824885989489, 3.7162593094967464]],
    [[0.0, 0.5], [0.6767230009741291, 0.75], [1.0, 1.2668995343135907], [1.6244882778609058, 1.75], [2.1772854270325794, 2.430761940989174], [2.640286836685923, 3.0], [3.411816899315357, 3.545577257021955], [3.7467714995306727, 3.6597220473041556]],
]
ROUTE = (1.125, 0.007674667287227956, 0.4193835330241189, 0.25, 6075, DUE)


def chunk_groups():
    return list(range(NV)) + list(range(2 * NV, CHUNKS)), list(range(NV, 2 * NV))


def plan_routes(rare, rarer, reach_weight, noise, seed, due):
    draw = np.random.RandomState(seed)
    nodes = [(x, z, q) for x in range(NX) for z in range(NZ) for q in range(NQ)]
    index = {n: i for i, n in enumerate(nodes)}
    count, items, never = len(nodes), LAYERS * CHUNKS, 999
    goes = np.array([
        [index[((x + 1) % NX, z, q)], index[((x - 1) % NX, z, q)],
         index[(x, (z + 1) % NZ, q)], index[(x, (z - 1) % NZ, q)], index[(x, z, 1 - q)]]
        for x, z, q in nodes
    ])
    layer, part = np.arange(items) // CHUNKS, np.arange(items) % CHUNKS
    group = ((part >= NV) & (part < 2 * NV)).astype(int)
    slab = np.array([z // NK for _, z, _ in nodes])
    when = np.full((count, items), never)
    for u, (x, z, q) in enumerate(nodes):
        when[u, layer == z // NK * NX + x] = 0
    urgency = np.array(due)[:, layer, group]
    sends = []
    while (when == never).any():
        r = len(sends)
        reached, far = when < never, np.zeros(items)
        copies = reached.sum(0) / count
        for _ in range(8):
            if reached.all():
                break
            far += ~reached.all(0)
            wider = reached.copy()
            for o in range(LINKS):
                wider[goes[:, o]] |= reached
            reached = wider
        keys = (urgency + copies * (rare + rarer * r) - far * reach_weight)[slab]
        jitter = draw.random_sample((count * LINKS, items)) * noise
        held, free = when <= r, when == never
        row = [[NONE] * LINKS for _ in nodes]
        for i in draw.permutation(count * LINKS):
            u, o = divmod(int(i), LINKS)
            v = goes[u, o]
            key = np.where(held[u] & free[v], keys[v] + jitter[i], 1e9)
            best = int(key.argmin())
            if key[best] < 1e8:
                free[v, best] = False
                when[v, best] = r + LAG
                row[u][o] = best % CHUNKS * LAYERS + best // CHUNKS
        sends.append(row)
    return nodes, goes, sends, [int(t) for t in when.max(0)]


def route_tables():
    nodes, goes, sends, ready = plan_routes(*ROUTE)
    rounds = len(sends) + LAG
    back = [1, 0, 3, 2, 4]
    out_table = [[[NONE] * LINKS for _ in nodes] for _ in range(rounds)]
    in_table = [[[NONE] * LINKS for _ in nodes] for _ in range(rounds)]
    for r, row in enumerate(sends):
        for u in range(len(nodes)):
            for o in range(LINKS):
                out_table[r][u][o] = row[u][o]
                in_table[r + LAG][goes[u][o]][back[o]] = row[u][o]
    return nodes, out_table, in_table, step_rounds(ready)


def step_rounds(ready):
    def last_of(layer, group):
        return max(ready[layer * CHUNKS + c] for c in group)

    first, second = chunk_groups()
    starts, at = [], -1
    for layer in range(LAYERS + 1):
        need = last_of(layer, first) if layer < LAYERS else 0
        if layer:
            need = max(need, last_of(layer - 1, second))
        at = max(at + PACE, need)
        starts.append(int(at))
        at += PACE
        starts.append(int(at))
    return starts


def kernel(
    tables, v_hbm, u_hbm, c_hbm, gate_ref, bias_ref, feat_hbm, out_hbm,
    W, E, X0, XC, ACC, DACC, PS, PR, DS, DR, T_OUT, T_IN,
    local_sem, w_recv, e_recv, wd_recv, ed_recv, w_send, e_send, wd_send, ed_send,
    x_sem, p_send, p_recv, d_send, d_recv, o_local, o_send, o_recv,
):
    nodes, out_table, in_table, starts = tables
    rounds = len(out_table)
    total = max(rounds, starts[-1] + 1)
    rows, half = X0.shape[1], X0.shape[2]
    sub_cols, piece = half // 2, half // 4
    rank = piece // 2
    block = rows // 2
    deep = piece // PART

    sec = lax.axis_index("section")
    dp = lax.axis_index("dp")
    x, h = sec % NX, sec // NX
    core, y, k = dp % 2, dp // 2 % NY, dp // (2 * NY)
    z = h * NK + k
    q = 1 - y % 2
    p = (y + 1) // 2 % 2
    mine = y % 2
    pair_y = y + 1 - 2 * mine
    share_y = (y + 1 - 2 * q + NY) % NY

    def device(x_, z_, y_, core_):
        return (z_ // NK * NX + x_, (z_ % NK * NY + y_) * 2 + core_)

    targets = [
        device((x + 1) % NX, z, y, core), device((x + NX - 1) % NX, z, y, core),
        device(x, (z + 1) % NZ, y, core), device(x, (z + NZ - 1) % NZ, y, core),
        device(x, z, share_y, core),
    ]
    pair = device(x, z, pair_y, core)
    sibling = device(x, z, y, 1 - core)

    def local(src, dst, sem):
        return pltpu.make_async_copy(src, dst, sem)

    def remote(src, dst, send, recv, to):
        return pltpu.make_async_remote_copy(
            src_ref=src, dst_ref=dst, send_sem=send, recv_sem=recv, device_id=to, device_id_type=MESH
        )

    def arrived(ref, sem):
        pltpu.make_async_copy(ref, ref, sem).wait()

    barrier = pltpu.get_barrier_semaphore()
    for to in targets + [pair, sibling]:
        pl.semaphore_signal(barrier, inc=1, device_id=to, device_id_type=MESH)

    base = pl.multiple_of(p * half, half)
    other = pl.multiple_of((1 - p) * half, half)
    own = []
    for s in range(2):
        for j in range(NV):
            own.append(local(
                v_hbm.at[0, pl.ds(pl.multiple_of(base + s * sub_cols + j * PART, PART), PART), :],
                W.at[s, j, sec], local_sem.at[s, j]))
            b, a = j // deep, j % deep
            own.append(local(
                u_hbm.at[0, a * PART:(a + 1) * PART, pl.ds(pl.multiple_of(base + s * sub_cols + b * piece, piece), piece)],
                W.at[s, NV + j, sec], local_sem.at[s, NV + j]))
        for j in range(NC):
            for e in range(2):
                own.append(local(
                    c_hbm.at[0, e, s * 128 + j * PART:s * 128 + (j + 1) * PART, :],
                    W.at[s, 2 * NV + j, sec, :, e * rank:(e + 1) * rank], local_sem.at[s, 2 * NV + 2 * j + e]))
    for copy in own:
        copy.start()
    x_local = [
        local(feat_hbm.at[0, 0, s * block:(s + 1) * block, pl.ds(base, half)],
              X0.at[s, pl.ds(pl.multiple_of(mine * block, block), block), :], x_sem.at[s])
        for s in range(2)
    ]
    for copy in x_local:
        copy.start()
    for s in range(2):
        extra = []
        for ref in (bias_ref, gate_ref):
            for b in range(2):
                cols = pl.ds(pl.multiple_of(base + s * sub_cols + b * piece, piece), piece)
                if ref is bias_ref:
                    extra.append(ref[0:1, cols])
                else:
                    both = ref[0, :, cols].astype(jnp.float32)
                    extra.append(both[0:1, :] - both[1:2, :])
        extra.append(jnp.zeros((4, piece), jnp.float32))
        E[s, sec] = jnp.concatenate(extra, axis=0)

    bits = [x % 2 == 1, x // 2 == 1, h == 1, q == 1, k // 2 == 1]
    shift = k % 2 * 16

    def lookup(table, r, o):
        values = {n: table[r][i][o] for i, n in enumerate(nodes)}
        level = []
        for cls in range(32):
            x_, h_, q_, k_ = cls % 4, cls // 4 % 2, cls // 8 % 2, cls // 16 * 2
            level.append(values[(x_, h_ * NK + k_, q_)] + (values[(x_, h_ * NK + k_ + 1, q_)] << 16))
        for bit in bits:
            level = [
                level[i] if isinstance(level[i], int) and isinstance(level[i + 1], int) and level[i] == level[i + 1]
                else jnp.where(bit, jnp.int32(level[i + 1]), jnp.int32(level[i]))
                for i in range(0, len(level), 2)
            ]
        word = level[0]
        if isinstance(word, int):
            word = jnp.int32(word)
        return lax.shift_right_logical(word, shift) & 4095

    for r in range(rounds):
        for o in range(LINKS):
            T_OUT[r * LINKS + o] = lookup(out_table, r, o)
            T_IN[r * LINKS + o] = lookup(in_table, r, o)

    pl.semaphore_wait(barrier, LINKS + 2)
    x_remote = [
        remote(feat_hbm.at[0, 0, s * block:(s + 1) * block, pl.ds(other, half)],
               X0.at[s, pl.ds(pl.multiple_of(mine * block, block), block), :], x_sem.at[2 + s], x_sem.at[4 + s], pair)
        for s in range(2)
    ]
    for copy in x_remote:
        copy.start()
    for copy in own:
        copy.wait()

    def settle(send_w, send_e, slot, ident):
        @pl.when(ident != NONE)
        def _():
            j, l = ident // LAYERS, ident % LAYERS
            arrived(W.at[core, j, l], send_w.at[slot])

            @pl.when(j == 2 * NV)
            def _():
                arrived(E.at[core, l], send_e.at[slot])

    def push(ident, slot, send_w, send_e, recv_w, recv_e, to):
        j, l = ident // LAYERS, ident % LAYERS
        remote(W.at[core, j, l], W.at[core, j, l], send_w.at[slot], recv_w.at[j, l], to).start()

        @pl.when(j == 2 * NV)
        def _():
            remote(E.at[core, l], E.at[core, l], send_e.at[slot], recv_e.at[l], to).start()

    def traffic(r):
        slot0 = r % SLOTS * LINKS
        came = [T_IN[r * LINKS + o] for o in range(LINKS)]
        for o in range(LINKS):
            @pl.when(came[o] != NONE)
            def _():
                j, l = came[o] // LAYERS, came[o] % LAYERS
                arrived(W.at[core, j, l], w_recv.at[j, l])

                @pl.when(j == 2 * NV)
                def _():
                    arrived(E.at[core, l], e_recv.at[l])

        for o in range(LINKS):
            goes_out = T_OUT[r * LINKS + o]

            @pl.when(goes_out != NONE)
            def _():
                push(goes_out, slot0 + o, w_send, e_send, w_recv, e_recv, targets[o])

        for o in range(LINKS):
            @pl.when(came[o] != NONE)
            def _():
                push(came[o], slot0 + o, wd_send, ed_send, wd_recv, ed_recv, sibling)

    def settle_round(r):
        for o in range(LINKS):
            slot = r % SLOTS * LINKS + o
            settle(w_send, e_send, slot, T_OUT[r * LINKS + o])
            settle(wd_send, ed_send, slot, T_IN[r * LINKS + o])

    def weights_here(l, low, high, extra=False):
        @pl.when(l != sec)
        def _():
            def one(j, carry):
                arrived(W.at[1 - core, j, l], wd_recv.at[j, l])
                return carry
            lax.fori_loop(low, high, one, 0)
            if extra:
                arrived(E.at[1 - core, l], ed_recv.at[l])

    def project(l, s):
        acc = jnp.zeros((rows, piece), jnp.float32)
        mixed = jnp.zeros((rows, piece), jnp.float32)
        for sub in range(2):
            part = XC[s, :, sub * sub_cols:(sub + 1) * sub_cols]
            v_mat = W[sub, 0:NV, l].reshape(sub_cols, piece)
            acc = acc + jnp.dot(part, v_mat, preferred_element_type=jnp.float32)
            for b in range(2):
                cut = part[:, b * piece:(b + 1) * piece].astype(jnp.float32)
                mixed = mixed + cut * E[sub, l, 2 + b:3 + b, :]
        ACC[s] = acc
        PS[l, s] = acc.astype(jnp.bfloat16)
        lanes = mixed[:, 0:128] + mixed[:, 128:256] + mixed[:, 256:384] + mixed[:, 384:512]
        logit = jnp.broadcast_to(jnp.sum(lanes, axis=1, keepdims=True), (rows, 128))
        DACC[s] = logit
        DS[l, s] = logit.T[0:8, :]
        remote(PS.at[l, s], PR.at[l, s], p_send.at[l, s], p_recv.at[l, s], pair).start()
        remote(DS.at[l, s], DR.at[l, s], d_send.at[l, s], d_recv.at[l, s], pair).start()

    def blend(l, s):
        arrived(PR.at[l, s], p_recv.at[l, s])
        arrived(DR.at[l, s], d_recv.at[l, s])
        first = jnp.tanh(ACC[s] + PR[l, s].astype(jnp.float32)).astype(jnp.bfloat16)
        logit = DACC[s] + jnp.broadcast_to(DR[l, s][0:1, :], (128, rows)).T
        gates = (1.0 / (1.0 + jnp.exp(-logit)), 1.0 / (1.0 + jnp.exp(logit)))
        c_mat = W[:, 2 * NV:CHUNKS, l].reshape(rank, piece)
        parts = []
        for i in range(2):
            cols = slice(i * rank, (i + 1) * rank)
            second = jnp.dot(first[:, cols], c_mat[:, cols], preferred_element_type=jnp.float32)
            gate = jnp.concatenate([gates[i], gates[i]], axis=1)
            parts.append((gate * jnp.tanh(second)).astype(jnp.bfloat16))
        return jnp.concatenate(parts, axis=1)

    def results(b, s, sub):
        at = sub * sub_cols + b * piece
        src = slice(at, at + piece)
        dst = out_hbm.at[0, 0, pl.ds(pl.multiple_of(s * block, block), block), pl.ds(pl.multiple_of(base + at, piece), piece)]
        slot = b * 4 + s * 2 + sub
        return remote(
            XC.at[s, pl.ds(pl.multiple_of((1 - mine) * block, block), block), src], dst,
            o_send.at[slot], o_recv.at[slot], pair)

    def keep(b, s, sub):
        at = sub * sub_cols + b * piece
        own_rows = XC[s, pl.ds(pl.multiple_of(mine * block, block), block), at:at + piece]
        out_hbm[0, 0, pl.ds(pl.multiple_of(s * block, block), block), pl.ds(pl.multiple_of(base + at, piece), piece)] = own_rows

    def finish(l, s):
        blended = blend(l, s)
        for b in range(2):
            for sub in range(2):
                u_mat = W[sub, NV + deep * b:NV + deep * (b + 1), l].reshape(piece, piece)
                cross = jnp.dot(blended, u_mat, preferred_element_type=jnp.float32)
                at = sub * sub_cols + b * piece
                cols = slice(at, at + piece)
                new = XC[s, :, cols].astype(jnp.float32) + X0[s, :, cols].astype(jnp.float32) * (
                    cross + E[sub, l, b:b + 1, :])
                XC[s, :, cols] = new.astype(jnp.bfloat16)

                @pl.when(l == LAYERS - 1)
                def _():
                    results(b, s, sub).start()
                    keep(b, s, sub)

    def one_round(r, carry):
        @pl.when(r < rounds)
        def _():
            traffic(r)

        step = jnp.int32(-1)
        fires = jnp.int32(0)
        for start in starts:
            step = step + jnp.where(r >= start, 1, 0)
            fires = fires + jnp.where(r == start, 1, 0)

        @pl.when(fires > 0)
        def _():
            l, s = step // 2, step % 2

            @pl.when(step == 0)
            def _():
                for copy in x_local:
                    copy.wait()
                for s_ in range(2):
                    x_remote[s_].wait_send()
                    arrived(X0.at[s_, pl.ds(pl.multiple_of((1 - mine) * block, block), block), :], x_sem.at[4 + s_])
                XC[...] = X0[...]

            @pl.when(step >= 2)
            def _():
                @pl.when(s == 0)
                def _():
                    weights_here(l - 1, NV, 2 * NV)
                finish(l - 1, s)

            @pl.when(l < LAYERS)
            def _():
                @pl.when(s == 0)
                def _():
                    weights_here(l, 0, NV)
                    weights_here(l, 2 * NV, CHUNKS, True)
                project(l, s)

        @pl.when((r >= SLOTS - 1) & (r < rounds))
        def _():
            settle_round(r - (SLOTS - 1))

        return carry

    lax.fori_loop(0, total, one_round, 0)

    def last_rounds(r, carry):
        settle_round(r)
        return carry

    lax.fori_loop(rounds - (SLOTS - 1), rounds, last_rounds, 0)

    def sent(i, carry):
        l, s = i // 2, i % 2
        arrived(PS.at[l, s], p_send.at[l, s])
        arrived(DS.at[l, s], d_send.at[l, s])
        return carry

    lax.fori_loop(0, LAYERS * 2, sent, 0)
    for b in range(2):
        for s in range(2):
            for sub in range(2):
                results(b, jnp.int32(s), sub).wait_send()
                at = sub * sub_cols + b * piece
                arrived(out_hbm.at[0, 0, s * block:(s + 1) * block, pl.ds(pl.multiple_of(other + at, piece), piece)],
                        o_recv.at[b * 4 + s * 2 + sub])


def per_device(features, in_proj, mix_proj, out_proj, gate_proj, cross_bias):
    rows, width = features.shape[2], features.shape[3]
    experts, rank = mix_proj.shape[1], mix_proj.shape[2]
    half, piece = width // 2, experts * rank
    tables = route_tables()
    rounds = len(tables[1])
    any_space = pl.BlockSpec(memory_space=pl.ANY)
    dma = pltpu.SemaphoreType.DMA
    return pl.pallas_call(
        functools.partial(kernel, tables),
        out_shape=pltpu.VMEM(features.shape, features.dtype),
        in_specs=[any_space] * 3 + [pl.BlockSpec(memory_space=pltpu.VMEM)] * 2 + [any_space],
        out_specs=pl.BlockSpec(memory_space=pltpu.VMEM),
        scratch_shapes=[
            pltpu.VMEM((2, CHUNKS, LAYERS, PART, piece), jnp.bfloat16),
            pltpu.VMEM((2, LAYERS, 8, piece), jnp.float32),
            pltpu.VMEM((2, rows, half), jnp.bfloat16),
            pltpu.VMEM((2, rows, half), jnp.bfloat16),
            pltpu.VMEM((2, rows, piece), jnp.float32),
            pltpu.VMEM((2, rows, 128), jnp.float32),
            pltpu.VMEM((LAYERS, 2, rows, piece), jnp.bfloat16),
            pltpu.VMEM((LAYERS, 2, rows, piece), jnp.bfloat16),
            pltpu.VMEM((LAYERS, 2, 8, rows), jnp.float32),
            pltpu.VMEM((LAYERS, 2, 8, rows), jnp.float32),
            pltpu.SMEM((rounds * LINKS,), jnp.int32),
            pltpu.SMEM((rounds * LINKS,), jnp.int32),
            dma((2, CHUNKS + NC)),
            dma((CHUNKS, LAYERS)), dma((LAYERS,)),
            dma((CHUNKS, LAYERS)), dma((LAYERS,)),
            dma((SLOTS * LINKS,)), dma((SLOTS * LINKS,)),
            dma((SLOTS * LINKS,)), dma((SLOTS * LINKS,)),
            dma((6,)),
            dma((LAYERS, 2)), dma((LAYERS, 2)), dma((LAYERS, 2)), dma((LAYERS, 2)),
            dma((8,)), dma((8,)), dma((8,)),
        ],
        compiler_params=pltpu.CompilerParams(
            collective_id=0, has_side_effects=True, vmem_limit_bytes=60 * 1024 * 1024
        ),
    )(in_proj, out_proj, mix_proj, gate_proj, cross_bias, features)


def solution(mesh):
    placed = (
        P(None, "section", "dp", None),
        P("section", None, None),
        P("section", None, None, None),
        P("section", None, None),
        P("section", None, None),
        P("section", None),
    )
    return jax.shard_map(
        per_device,
        mesh=mesh,
        in_specs=placed,
        out_specs=P(None, "section", "dp", None),
        check_vma=False,
    )
```

```python
import functools

import jax
import jax.numpy as jnp
import numpy as np
from jax import lax
from jax.experimental import pallas as pl
from jax.experimental.pallas import tpu as pltpu
from jax.sharding import PartitionSpec as P

MESH = pl.DeviceIdType.MESH
NX, NH, NK, NY, NQ = 4, 2, 4, 4, 2
NZ = NH * NK
LAYERS = NX * NH
PART = 128
NV = 1024 // PART
NC = 128 // PART
CHUNKS = 2 * NV + NC
LINKS = 5
LAG = 2
PACE = 1.0
SLOTS = 4
NONE = 4095
DUE = [
    [[0.0, 0.5], [0.5849288578929801, 1.2859887393727676], [0.9381583654646382, 1.1455558452467394], [1.3719483597663404, 1.6804870085712993], [2.049650217767926, 2.430761940989174], [2.640286836685923, 2.621520203407922], [3.08954911142396, 3.24213595349004], [3.303594641293013, 4.2123413743513884]],
    [[0.0, 0.7683993199339043], [0.6767230009741291, 0.75], [1.0, 1.0688809251609854], [1.3719483597663404, 1.7424364088176243], [1.931100771933383, 2.516083922725886], [2.7223144702913498, 2.621520203407922], [3.411816899315357, 3.545577257021955], [3.7238975877989575, 4.430260712247482]],
]
ROUTE = (1.125, 0.007674667287227956, 0.26778480630314494, 0.25, 6834, DUE)


def chunk_groups():
    return list(range(NV)) + list(range(2 * NV, CHUNKS)), list(range(NV, 2 * NV))


def plan_routes(rare, rarer, reach_weight, noise, seed, due):
    draw = np.random.RandomState(seed)
    nodes = [(x, z, q) for x in range(NX) for z in range(NZ) for q in range(NQ)]
    index = {n: i for i, n in enumerate(nodes)}
    count, items, never = len(nodes), LAYERS * CHUNKS, 999
    goes = np.array([
        [index[((x + 1) % NX, z, q)], index[((x - 1) % NX, z, q)],
         index[(x, (z + 1) % NZ, q)], index[(x, (z - 1) % NZ, q)], index[(x, z, 1 - q)]]
        for x, z, q in nodes
    ])
    layer, part = np.arange(items) // CHUNKS, np.arange(items) % CHUNKS
    group = ((part >= NV) & (part < 2 * NV)).astype(int)
    slab = np.array([z // NK for _, z, _ in nodes])
    when = np.full((count, items), never)
    for u, (x, z, q) in enumerate(nodes):
        when[u, layer == z // NK * NX + x] = 0
    urgency = np.array(due)[:, layer, group]
    sends = []
    while (when == never).any():
        r = len(sends)
        reached, far = when < never, np.zeros(items)
        copies = reached.sum(0) / count
        for _ in range(8):
            if reached.all():
                break
            far += ~reached.all(0)
            wider = reached.copy()
            for o in range(LINKS):
                wider[goes[:, o]] |= reached
            reached = wider
        keys = (urgency + copies * (rare + rarer * r) - far * reach_weight)[slab]
        jitter = draw.random_sample((count * LINKS, items)) * noise
        held, free = when <= r, when == never
        row = [[NONE] * LINKS for _ in nodes]
        for i in draw.permutation(count * LINKS):
            u, o = divmod(int(i), LINKS)
            v = goes[u, o]
            key = np.where(held[u] & free[v], keys[v] + jitter[i], 1e9)
            best = int(key.argmin())
            if key[best] < 1e8:
                free[v, best] = False
                when[v, best] = r + LAG
                row[u][o] = best % CHUNKS * LAYERS + best // CHUNKS
        sends.append(row)
    return nodes, goes, sends, [int(t) for t in when.max(0)]


def route_tables():
    nodes, goes, sends, ready = plan_routes(*ROUTE)
    rounds = len(sends) + LAG
    back = [1, 0, 3, 2, 4]
    out_table = [[[NONE] * LINKS for _ in nodes] for _ in range(rounds)]
    in_table = [[[NONE] * LINKS for _ in nodes] for _ in range(rounds)]
    for r, row in enumerate(sends):
        for u in range(len(nodes)):
            for o in range(LINKS):
                out_table[r][u][o] = row[u][o]
                in_table[r + LAG][goes[u][o]][back[o]] = row[u][o]
    return nodes, out_table, in_table, step_rounds(ready)


def step_rounds(ready):
    def last_of(layer, group):
        return max(ready[layer * CHUNKS + c] for c in group)

    first, second = chunk_groups()
    starts, at = [], -1
    for layer in range(LAYERS + 1):
        need = last_of(layer, first) if layer < LAYERS else 0
        if layer:
            need = max(need, last_of(layer - 1, second))
        at = max(at + PACE, need)
        starts.append(int(at))
        at += PACE
        starts.append(int(at))
    return starts


def kernel(
    tables, v_hbm, u_hbm, c_hbm, gate_ref, bias_ref, feat_hbm, out_hbm,
    W, E, X0, XC, ACC, DACC, PS, PR, DS, DR, T_OUT, T_IN,
    local_sem, w_recv, e_recv, wd_recv, ed_recv, w_send, e_send, wd_send, ed_send,
    x_sem, p_send, p_recv, d_send, d_recv, o_local, o_send, o_recv,
):
    nodes, out_table, in_table, starts = tables
    rounds = len(out_table)
    total = max(rounds, starts[-1] + 1)
    rows, half = X0.shape[1], X0.shape[2]
    sub_cols, piece = half // 2, half // 4
    rank = piece // 2
    block = rows // 2
    deep = piece // PART

    sec = lax.axis_index("section")
    dp = lax.axis_index("dp")
    x, h = sec % NX, sec // NX
    core, y, k = dp % 2, dp // 2 % NY, dp // (2 * NY)
    z = h * NK + k
    q = 1 - y % 2
    p = (y + 1) // 2 % 2
    mine = y % 2
    pair_y = y + 1 - 2 * mine
    share_y = (y + 1 - 2 * q + NY) % NY

    def device(x_, z_, y_, core_):
        return (z_ // NK * NX + x_, (z_ % NK * NY + y_) * 2 + core_)

    targets = [
        device((x + 1) % NX, z, y, core), device((x + NX - 1) % NX, z, y, core),
        device(x, (z + 1) % NZ, y, core), device(x, (z + NZ - 1) % NZ, y, core),
        device(x, z, share_y, core),
    ]
    pair = device(x, z, pair_y, core)
    sibling = device(x, z, y, 1 - core)

    def local(src, dst, sem):
        return pltpu.make_async_copy(src, dst, sem)

    def remote(src, dst, send, recv, to):
        return pltpu.make_async_remote_copy(
            src_ref=src, dst_ref=dst, send_sem=send, recv_sem=recv, device_id=to, device_id_type=MESH
        )

    def arrived(ref, sem):
        pltpu.make_async_copy(ref, ref, sem).wait()

    barrier = pltpu.get_barrier_semaphore()
    for to in targets + [pair, sibling]:
        pl.semaphore_signal(barrier, inc=1, device_id=to, device_id_type=MESH)

    base = pl.multiple_of(p * half, half)
    other = pl.multiple_of((1 - p) * half, half)
    own = []
    for s in range(2):
        for j in range(NV):
            own.append(local(
                v_hbm.at[0, pl.ds(pl.multiple_of(base + s * sub_cols + j * PART, PART), PART), :],
                W.at[s, j, sec], local_sem.at[s, j]))
            b, a = j // deep, j % deep
            own.append(local(
                u_hbm.at[0, a * PART:(a + 1) * PART, pl.ds(pl.multiple_of(base + s * sub_cols + b * piece, piece), piece)],
                W.at[s, NV + j, sec], local_sem.at[s, NV + j]))
        for j in range(NC):
            for e in range(2):
                own.append(local(
                    c_hbm.at[0, e, s * 128 + j * PART:s * 128 + (j + 1) * PART, :],
                    W.at[s, 2 * NV + j, sec, :, e * rank:(e + 1) * rank], local_sem.at[s, 2 * NV + 2 * j + e]))
    for copy in own:
        copy.start()
    x_local = [
        local(feat_hbm.at[0, 0, s * block:(s + 1) * block, pl.ds(base, half)],
              X0.at[s, pl.ds(pl.multiple_of(mine * block, block), block), :], x_sem.at[s])
        for s in range(2)
    ]
    for copy in x_local:
        copy.start()
    for s in range(2):
        extra = []
        for ref in (bias_ref, gate_ref):
            for b in range(2):
                cols = pl.ds(pl.multiple_of(base + s * sub_cols + b * piece, piece), piece)
                if ref is bias_ref:
                    extra.append(ref[0:1, cols])
                else:
                    both = ref[0, :, cols].astype(jnp.float32)
                    extra.append(both[0:1, :] - both[1:2, :])
        extra.append(jnp.zeros((4, piece), jnp.float32))
        E[s, sec] = jnp.concatenate(extra, axis=0)

    bits = [x % 2 == 1, x // 2 == 1, h == 1, q == 1, k // 2 == 1]
    shift = k % 2 * 16

    def lookup(table, r, o):
        values = {n: table[r][i][o] for i, n in enumerate(nodes)}
        level = []
        for cls in range(32):
            x_, h_, q_, k_ = cls % 4, cls // 4 % 2, cls // 8 % 2, cls // 16 * 2
            level.append(values[(x_, h_ * NK + k_, q_)] + (values[(x_, h_ * NK + k_ + 1, q_)] << 16))
        for bit in bits:
            level = [
                level[i] if isinstance(level[i], int) and isinstance(level[i + 1], int) and level[i] == level[i + 1]
                else jnp.where(bit, jnp.int32(level[i + 1]), jnp.int32(level[i]))
                for i in range(0, len(level), 2)
            ]
        word = level[0]
        if isinstance(word, int):
            word = jnp.int32(word)
        return lax.shift_right_logical(word, shift) & 4095

    for r in range(rounds):
        for o in range(LINKS):
            T_OUT[r * LINKS + o] = lookup(out_table, r, o)
            T_IN[r * LINKS + o] = lookup(in_table, r, o)

    pl.semaphore_wait(barrier, LINKS + 2)
    x_remote = [
        remote(feat_hbm.at[0, 0, s * block:(s + 1) * block, pl.ds(other, half)],
               X0.at[s, pl.ds(pl.multiple_of(mine * block, block), block), :], x_sem.at[2 + s], x_sem.at[4 + s], pair)
        for s in range(2)
    ]
    for copy in x_remote:
        copy.start()
    for copy in own:
        copy.wait()

    def settle(send_w, send_e, slot, ident):
        @pl.when(ident != NONE)
        def _():
            j, l = ident // LAYERS, ident % LAYERS
            arrived(W.at[core, j, l], send_w.at[slot])

            @pl.when(j == 2 * NV)
            def _():
                arrived(E.at[core, l], send_e.at[slot])

    def push(ident, slot, send_w, send_e, recv_w, recv_e, to):
        j, l = ident // LAYERS, ident % LAYERS
        remote(W.at[core, j, l], W.at[core, j, l], send_w.at[slot], recv_w.at[j, l], to).start()

        @pl.when(j == 2 * NV)
        def _():
            remote(E.at[core, l], E.at[core, l], send_e.at[slot], recv_e.at[l], to).start()

    def traffic(r):
        slot0 = r % SLOTS * LINKS
        came = [T_IN[r * LINKS + o] for o in range(LINKS)]
        for o in range(LINKS):
            @pl.when(came[o] != NONE)
            def _():
                j, l = came[o] // LAYERS, came[o] % LAYERS
                arrived(W.at[core, j, l], w_recv.at[j, l])

                @pl.when(j == 2 * NV)
                def _():
                    arrived(E.at[core, l], e_recv.at[l])

        for o in range(LINKS):
            goes_out = T_OUT[r * LINKS + o]

            @pl.when(goes_out != NONE)
            def _():
                push(goes_out, slot0 + o, w_send, e_send, w_recv, e_recv, targets[o])

        for o in range(LINKS):
            @pl.when(came[o] != NONE)
            def _():
                push(came[o], slot0 + o, wd_send, ed_send, wd_recv, ed_recv, sibling)

    def settle_round(r):
        for o in range(LINKS):
            slot = r % SLOTS * LINKS + o
            settle(w_send, e_send, slot, T_OUT[r * LINKS + o])
            settle(wd_send, ed_send, slot, T_IN[r * LINKS + o])

    def weights_here(l, low, high, extra=False):
        @pl.when(l != sec)
        def _():
            def one(j, carry):
                arrived(W.at[1 - core, j, l], wd_recv.at[j, l])
                return carry
            lax.fori_loop(low, high, one, 0)
            if extra:
                arrived(E.at[1 - core, l], ed_recv.at[l])

    def project(l, s):
        acc = jnp.zeros((rows, piece), jnp.float32)
        mixed = jnp.zeros((rows, piece), jnp.float32)
        for sub in range(2):
            part = XC[s, :, sub * sub_cols:(sub + 1) * sub_cols]
            v_mat = W[sub, 0:NV, l].reshape(sub_cols, piece)
            acc = acc + jnp.dot(part, v_mat, preferred_element_type=jnp.float32)
            for b in range(2):
                cut = part[:, b * piece:(b + 1) * piece].astype(jnp.float32)
                mixed = mixed + cut * E[sub, l, 2 + b:3 + b, :]
        ACC[s] = acc
        PS[l, s] = acc.astype(jnp.bfloat16)
        lanes = mixed[:, 0:128] + mixed[:, 128:256] + mixed[:, 256:384] + mixed[:, 384:512]
        logit = jnp.broadcast_to(jnp.sum(lanes, axis=1, keepdims=True), (rows, 128))
        DACC[s] = logit
        DS[l, s] = logit.T[0:8, :]
        remote(PS.at[l, s], PR.at[l, s], p_send.at[l, s], p_recv.at[l, s], pair).start()
        remote(DS.at[l, s], DR.at[l, s], d_send.at[l, s], d_recv.at[l, s], pair).start()

    def blend(l, s):
        arrived(PR.at[l, s], p_recv.at[l, s])
        arrived(DR.at[l, s], d_recv.at[l, s])
        first = jnp.tanh(ACC[s] + PR[l, s].astype(jnp.float32)).astype(jnp.bfloat16)
        logit = DACC[s] + jnp.broadcast_to(DR[l, s][0:1, :], (128, rows)).T
        gates = (1.0 / (1.0 + jnp.exp(-logit)), 1.0 / (1.0 + jnp.exp(logit)))
        c_mat = W[:, 2 * NV:CHUNKS, l].reshape(rank, piece)
        parts = []
        for i in range(2):
            cols = slice(i * rank, (i + 1) * rank)
            second = jnp.dot(first[:, cols], c_mat[:, cols], preferred_element_type=jnp.float32)
            gate = jnp.concatenate([gates[i], gates[i]], axis=1)
            parts.append((gate * jnp.tanh(second)).astype(jnp.bfloat16))
        return jnp.concatenate(parts, axis=1)

    def results(b, s, sub):
        at = sub * sub_cols + b * piece
        src = slice(at, at + piece)
        dst = out_hbm.at[0, 0, pl.ds(pl.multiple_of(s * block, block), block), pl.ds(pl.multiple_of(base + at, piece), piece)]
        slot = b * 4 + s * 2 + sub
        return remote(
            XC.at[s, pl.ds(pl.multiple_of((1 - mine) * block, block), block), src], dst,
            o_send.at[slot], o_recv.at[slot], pair)

    def keep(b, s, sub):
        at = sub * sub_cols + b * piece
        own_rows = XC[s, pl.ds(pl.multiple_of(mine * block, block), block), at:at + piece]
        out_hbm[0, 0, pl.ds(pl.multiple_of(s * block, block), block), pl.ds(pl.multiple_of(base + at, piece), piece)] = own_rows

    def finish(l, s):
        blended = blend(l, s)
        for b in range(2):
            for sub in range(2):
                u_mat = W[sub, NV + deep * b:NV + deep * (b + 1), l].reshape(piece, piece)
                cross = jnp.dot(blended, u_mat, preferred_element_type=jnp.float32)
                at = sub * sub_cols + b * piece
                cols = slice(at, at + piece)
                new = XC[s, :, cols].astype(jnp.float32) + X0[s, :, cols].astype(jnp.float32) * (
                    cross + E[sub, l, b:b + 1, :])
                XC[s, :, cols] = new.astype(jnp.bfloat16)

                @pl.when(l == LAYERS - 1)
                def _():
                    results(b, s, sub).start()
                    keep(b, s, sub)

    def one_round(r, carry):
        @pl.when(r < rounds)
        def _():
            traffic(r)

        step = jnp.int32(-1)
        fires = jnp.int32(0)
        for start in starts:
            step = step + jnp.where(r >= start, 1, 0)
            fires = fires + jnp.where(r == start, 1, 0)

        @pl.when(fires > 0)
        def _():
            l, s = step // 2, step % 2

            @pl.when(step == 0)
            def _():
                for copy in x_local:
                    copy.wait()
                for s_ in range(2):
                    x_remote[s_].wait_send()
                    arrived(X0.at[s_, pl.ds(pl.multiple_of((1 - mine) * block, block), block), :], x_sem.at[4 + s_])
                XC[...] = X0[...]

            @pl.when(step >= 2)
            def _():
                @pl.when(s == 0)
                def _():
                    weights_here(l - 1, NV, 2 * NV)
                finish(l - 1, s)

            @pl.when(l < LAYERS)
            def _():
                @pl.when(s == 0)
                def _():
                    weights_here(l, 0, NV)
                    weights_here(l, 2 * NV, CHUNKS, True)
                project(l, s)

        @pl.when((r >= SLOTS - 1) & (r < rounds))
        def _():
            settle_round(r - (SLOTS - 1))

        return carry

    lax.fori_loop(0, total, one_round, 0)

    def last_rounds(r, carry):
        settle_round(r)
        return carry

    lax.fori_loop(rounds - (SLOTS - 1), rounds, last_rounds, 0)

    def sent(i, carry):
        l, s = i // 2, i % 2
        arrived(PS.at[l, s], p_send.at[l, s])
        arrived(DS.at[l, s], d_send.at[l, s])
        return carry

    lax.fori_loop(0, LAYERS * 2, sent, 0)
    for b in range(2):
        for s in range(2):
            for sub in range(2):
                results(b, jnp.int32(s), sub).wait_send()
                at = sub * sub_cols + b * piece
                arrived(out_hbm.at[0, 0, s * block:(s + 1) * block, pl.ds(pl.multiple_of(other + at, piece), piece)],
                        o_recv.at[b * 4 + s * 2 + sub])


def per_device(features, in_proj, mix_proj, out_proj, gate_proj, cross_bias):
    rows, width = features.shape[2], features.shape[3]
    experts, rank = mix_proj.shape[1], mix_proj.shape[2]
    half, piece = width // 2, experts * rank
    tables = route_tables()
    rounds = len(tables[1])
    any_space = pl.BlockSpec(memory_space=pl.ANY)
    dma = pltpu.SemaphoreType.DMA
    return pl.pallas_call(
        functools.partial(kernel, tables),
        out_shape=pltpu.VMEM(features.shape, features.dtype),
        in_specs=[any_space] * 3 + [pl.BlockSpec(memory_space=pltpu.VMEM)] * 2 + [any_space],
        out_specs=pl.BlockSpec(memory_space=pltpu.VMEM),
        scratch_shapes=[
            pltpu.VMEM((2, CHUNKS, LAYERS, PART, piece), jnp.bfloat16),
            pltpu.VMEM((2, LAYERS, 8, piece), jnp.float32),
            pltpu.VMEM((2, rows, half), jnp.bfloat16),
            pltpu.VMEM((2, rows, half), jnp.bfloat16),
            pltpu.VMEM((2, rows, piece), jnp.float32),
            pltpu.VMEM((2, rows, 128), jnp.float32),
            pltpu.VMEM((LAYERS, 2, rows, piece), jnp.bfloat16),
            pltpu.VMEM((LAYERS, 2, rows, piece), jnp.bfloat16),
            pltpu.VMEM((LAYERS, 2, 8, rows), jnp.float32),
            pltpu.VMEM((LAYERS, 2, 8, rows), jnp.float32),
            pltpu.SMEM((rounds * LINKS,), jnp.int32),
            pltpu.SMEM((rounds * LINKS,), jnp.int32),
            dma((2, CHUNKS + NC)),
            dma((CHUNKS, LAYERS)), dma((LAYERS,)),
            dma((CHUNKS, LAYERS)), dma((LAYERS,)),
            dma((SLOTS * LINKS,)), dma((SLOTS * LINKS,)),
            dma((SLOTS * LINKS,)), dma((SLOTS * LINKS,)),
            dma((6,)),
            dma((LAYERS, 2)), dma((LAYERS, 2)), dma((LAYERS, 2)), dma((LAYERS, 2)),
            dma((8,)), dma((8,)), dma((8,)),
        ],
        compiler_params=pltpu.CompilerParams(
            collective_id=0, has_side_effects=True, vmem_limit_bytes=60 * 1024 * 1024
        ),
    )(in_proj, out_proj, mix_proj, gate_proj, cross_bias, features)


def solution(mesh):
    placed = (
        P(None, "section", "dp", None),
        P("section", None, None),
        P("section", None, None, None),
        P("section", None, None),
        P("section", None, None),
        P("section", None),
    )
    return jax.shard_map(
        per_device,
        mesh=mesh,
        in_specs=placed,
        out_specs=P(None, "section", "dp", None),
        check_vma=False,
    )
```
